32 devices in a mesh: batch: 4 (over z), frame: 4 (over x, core), space: 2 (over y).
Axes of the slice: x: 2, y: 2, z: 4, core: 2. Of those that a mesh axis runs over, the one named last changes fastest.
Arguments:
- queries: bfloat16 [32, 2, 8, 8, 1536], P(('batch', 'frame'), 'space'), parts along dimension 0, may hold values from -6 to 6
- keys: bfloat16 [32, 2, 8, 8, 1536], P(('batch', 'frame'), 'space'), parts along dimension 0, may hold values from -6 to 6
- values: bfloat16 [32, 2, 8, 8, 1536], P(('batch', 'frame'), 'space'), parts along dimension 0, may hold values from -6 to 6
- hidden: bfloat16 [32, 2, 8, 8, 3072], P(('batch', 'frame'), 'space'), parts along dimension 0, may hold values from -6 to 6
- control: bfloat16 [32, 2, 8, 8, 3072], P(('batch', 'frame'), 'space'), parts along dimension 0, may hold values from -4 to 4
- gate: bfloat16 [3072], replicated, may hold values from 0.5 to 3
- out_weight: bfloat16 [1536, 3072], P(('frame', 'space')), may hold values from -0.15625 to 0.15625
Outputs:
- output: bfloat16 [32, 2, 8, 8, 3072], P(('batch', 'frame'), 'space'), parts along dimension 0
The draws below stay inside these ranges and needn't reach their ends.
There are 4 independent parts, one for each index of `batch`. The reference program is written for one: setup_inputs(seed, part) draws one part's arguments, and reference() takes and returns one part's arrays. A program takes and returns all parts, laid end to end along the dimension named above; an argument that names none is the same for every part. Nothing has to cross between parts.
All inputs are finite; a program needn't handle non-finite values.
Results may differ from the reference program's by a relative error of at most 0.0034.
Values may be sent and summed in bfloat16 or wider, within the bound.
No kernel may reach another device: no remote copies, remote signals or barrier semaphores. Data moves between devices by JAX's collectives and lax.ppermute only.
A program may use at most 128 MiB of HBM per device.

```python
import math
import jax
import jax.numpy as jnp
from jax import lax

D = 3072
HEADS = 12
HEAD_DIM = 128
TILE_F = 2
TILE_S = 8
HC = 1536
FRAMES = 8
BOXES = 2
GRID_W = 2
GRID_H = 1
N_FRAME = 4


def draw_queries(key, part):
    drawn = 1.4 * jax.random.normal(jax.random.fold_in(key, 1), (FRAMES * BOXES * TILE_S * TILE_S, HEADS, HEAD_DIM), jnp.float32)
    drawn = jnp.clip(drawn, -6.0, 6.0)
    return drawn.reshape(FRAMES, BOXES, TILE_S, TILE_S, HEADS * HEAD_DIM).astype(jnp.bfloat16)


def draw_keys(key, part):
    drawn = 1.4 * jax.random.normal(jax.random.fold_in(key, 2), (FRAMES * BOXES * TILE_S * TILE_S, HEADS, HEAD_DIM), jnp.float32)
    drawn = jnp.clip(drawn, -6.0, 6.0)
    return drawn.reshape(FRAMES, BOXES, TILE_S, TILE_S, HEADS * HEAD_DIM).astype(jnp.bfloat16)


def block_scale(key, dims, pieces, low, high):
    level, own = 1.0, jax.random.fold_in(key, 6)
    for dim, shards_of in pieces:
        steps = jnp.exp(jax.random.uniform(jax.random.fold_in(own, dim), (shards_of,), jnp.float32, low / len(pieces), high / len(pieces)))
        level = level * jnp.repeat(steps, dims[dim] // shards_of).reshape([-1 if axis == dim else 1 for axis in range(len(dims))])
    return level


def noise(stream_key, extent, scale, limit, shards=(), held_as=jnp.bfloat16):
    values = scale * jax.random.normal(stream_key, extent, jnp.float32)
    if shards:
        values = values * block_scale(stream_key, extent, shards, -0.22, 0.18)
    return jnp.clip(values, -limit, limit).astype(held_as)


def setup_inputs(seed: int = 0, part: int = 0) -> dict:
    key_list = jax.random.split(jax.random.key(seed), 8)
    part_keys = jax.random.split(jax.random.fold_in(key_list[7], part), 8)
    return {
        "queries": draw_queries(jax.random.fold_in(jax.random.fold_in(key_list[7], part), 71), part),
        "keys": draw_keys(jax.random.fold_in(jax.random.fold_in(key_list[7], part), 71), part),
        "values": noise(part_keys[2], (FRAMES, BOXES, TILE_S, TILE_S, HC), 1.0, 6.0, ((0, 4), (1, 2))),
        "hidden": noise(part_keys[3], (FRAMES, BOXES, TILE_S, TILE_S, D), 1.0, 6.0, ((0, 4), (1, 2))),
        "control": noise(part_keys[4], (FRAMES, BOXES, TILE_S, TILE_S, D), 0.5, 4.0, ((0, 4), (1, 2))),
        "gate": jnp.clip(jnp.exp(jax.random.uniform(key_list[5], (D,), jnp.float32, math.log(0.5), math.log(3.0))), 0.5, 3.0).astype(jnp.bfloat16),
        "out_weight": noise(key_list[6], (HC, D), HC ** -0.5, 0.15625, ((0, 8),)),
    }


def to_tiles(array):
    shaped = array.reshape(N_FRAME, TILE_F, GRID_H, GRID_W, TILE_S, TILE_S, HEADS, HEAD_DIM)
    shaped = shaped.transpose(0, 2, 3, 1, 4, 5, 6, 7)
    return shaped.reshape(N_FRAME, GRID_H, GRID_W, TILE_F * TILE_S * TILE_S, HEADS, HEAD_DIM)


def reference(queries, keys, values, hidden, control, gate, out_weight):
    per_tile = TILE_F * TILE_S * TILE_S
    score_scale = HEAD_DIM ** -0.5
    query_tiles = to_tiles(queries)
    padding = ((1, 1), (1, 1), (1, 1), (0, 0), (0, 0), (0, 0))
    key_tiles = jnp.pad(to_tiles(keys), padding)
    value_tiles = jnp.pad(to_tiles(values), padding)
    present = jnp.pad(jnp.ones((N_FRAME, GRID_H, GRID_W), jnp.float32), 1)

    def one_tile(tile_number):
        frame_pos = (tile_number // (GRID_H * GRID_W)).astype(jnp.int32)
        height_pos = (tile_number // GRID_W % GRID_H).astype(jnp.int32)
        width_pos = (tile_number % GRID_W).astype(jnp.int32)
        zero_pos = jnp.zeros((), jnp.int32)
        starts = (frame_pos, height_pos, width_pos, zero_pos, zero_pos, zero_pos)
        window_shape = (3, 3, 3, per_tile, HEADS, HEAD_DIM)
        window_keys = lax.dynamic_slice(key_tiles, starts, window_shape).reshape(27 * per_tile, HEADS, HEAD_DIM)
        window_values = lax.dynamic_slice(value_tiles, starts, window_shape).reshape(27 * per_tile, HEADS, HEAD_DIM)
        window_live = lax.dynamic_slice(present, starts[:3], (3, 3, 3)).reshape(27)
        live_keys = jnp.repeat(window_live, per_tile) > 0.5
        own_queries = lax.dynamic_slice(query_tiles, starts[:3] + (zero_pos, zero_pos, zero_pos),
                                        (1, 1, 1, per_tile, HEADS, HEAD_DIM)).reshape(per_tile, HEADS, HEAD_DIM)
        scores = jnp.einsum("qhe,khe->hqk", own_queries.astype(jnp.float32), window_keys.astype(jnp.float32)) * score_scale
        masked = jnp.where(live_keys[None, None, :], scores, -1e30)
        row_max = jnp.max(masked, axis=2, keepdims=True)
        weights = jnp.where(live_keys[None, None, :], jnp.exp(masked - row_max), 0.0)
        row_total = jnp.sum(weights, axis=2)
        rounded = weights.astype(jnp.bfloat16)
        blended = jnp.einsum("hqk,khe->qhe", rounded.astype(jnp.float32), window_values.astype(jnp.float32))
        return (blended / jnp.transpose(row_total)[:, :, None]).astype(jnp.bfloat16)

    tile_numbers = jnp.arange(N_FRAME * GRID_H * GRID_W, dtype=jnp.int32)
    outputs = lax.map(one_tile, tile_numbers)
    outputs = outputs.reshape(N_FRAME, GRID_H, GRID_W, TILE_F, TILE_S, TILE_S, HC)
    attention = outputs.transpose(0, 3, 1, 2, 4, 5, 6).reshape(-1, HC)
    projected = jnp.dot(attention, out_weight, preferred_element_type=jnp.float32)
    result = hidden.reshape(-1, D).astype(jnp.float32) + gate.astype(jnp.float32)[None, :] * projected
    result = result + control.reshape(-1, D).astype(jnp.float32)
    return result.astype(jnp.bfloat16).reshape(FRAMES, BOXES, TILE_S, TILE_S, D)
```

```python
import jax
import jax.numpy as jnp
from jax import lax
from jax.experimental import pallas as pl
from jax.experimental.pallas import tpu as pltpu
from jax.sharding import PartitionSpec as P

HEAD_DIM = 128


def line_partner(position, count, parity):
    partner = ((position + parity) ^ 1) - parity
    return partner if 0 <= partner < count else None


def line_swap(axis, count, stride, parity):
    size = lax.axis_size(axis)
    pairs, valid = [], []
    for device in range(size):
        position = device // stride % count
        partner = line_partner(position, count, parity)
        valid.append(partner is not None)
        if partner is not None:
            pairs.append((device, device + (partner - position) * stride))
    here = lax.axis_index(axis)
    ok = jnp.int32(0)
    if all(valid):
        ok = jnp.int32(1)
    else:
        for device in range(size):
            if valid[device]:
                ok = ok | (here == device).astype(jnp.int32)
    return (lambda value: lax.ppermute(value, axis, pairs)), ok


def window_tiles(keys, values):
    space_count = lax.axis_size("space")
    grid_cols = min(4, space_count)
    grid_rows = space_count // grid_cols
    frames = lax.axis_size("frame")
    tiles = [(keys, values, jnp.int32(1))]
    for axis, count, stride in (("space", grid_cols, 1), ("space", grid_rows, grid_cols), ("frame", frames, 1)):
        found = list(tiles)
        for parity in range(min(2, count - 1)):
            swap, ok = line_swap(axis, count, stride, parity)
            for k, v, live in tiles:
                found.append((swap(k), swap(v), live & ok))
        tiles = found
    return tiles


def attention_body(*refs, tile_count, group, scale):
    live_ref, query_ref = refs[:2]
    key_refs = refs[2 : 2 + tile_count]
    value_refs = refs[2 + tile_count : 2 + 2 * tile_count]
    out_ref = refs[-1]
    for head in range(group):
        cols = slice(head * HEAD_DIM, (head + 1) * HEAD_DIM)
        query = query_ref[:, cols]
        scores = []
        for index in range(tile_count):
            raw = lax.dot_general(
                query, key_refs[index][:, cols], (((1,), (1,)), ((), ())), preferred_element_type=jnp.float32
            )
            scores.append(jnp.where(live_ref[index] > 0, raw * scale, -1e30))
        top = scores[0]
        for score in scores[1:]:
            top = jnp.maximum(top, score)
        row_max = jnp.max(top, axis=1, keepdims=True)
        total, blended = None, None
        for index in range(tile_count):
            weights = jnp.exp(scores[index] - row_max)
            part = jnp.dot(
                weights.astype(jnp.bfloat16), value_refs[index][:, cols], preferred_element_type=jnp.float32
            )
            total = weights if total is None else total + weights
            blended = part if blended is None else blended + part
        row_total = jnp.sum(total, axis=1, keepdims=True)
        out_ref[:, cols] = (blended / row_total).astype(jnp.bfloat16)


def attend(queries, tiles):
    rows, channels = queries.shape
    heads = channels // HEAD_DIM
    group = 3 if heads % 3 == 0 else 1
    width = group * HEAD_DIM
    live = jnp.stack([t[2] for t in tiles])
    block = pl.BlockSpec((rows, width), lambda h: (0, h))
    return pl.pallas_call(
        lambda *refs: attention_body(*refs, tile_count=len(tiles), group=group, scale=HEAD_DIM ** (-0.5)),
        grid=(heads // group,),
        in_specs=[pl.BlockSpec(memory_space=pltpu.SMEM)] + [block] * (1 + 2 * len(tiles)),
        out_specs=block,
        out_shape=jax.ShapeDtypeStruct((rows, channels), jnp.bfloat16),
        name="window_attention",
    )(live, queries, *[t[0] for t in tiles], *[t[1] for t in tiles])


def project_body(*refs, piece_counts, block_rows, has_acc, final):
    refs = list(refs)
    order_ref, attention_ref = refs[:2]
    refs = refs[2:]
    acc = None
    if has_acc:
        acc = refs.pop(0)[...]
    blocks_ref = refs.pop()
    out_ref = refs.pop()

    @pl.when(pl.program_id(0) == 0)
    def _():
        for index in range(attention_ref.shape[1] // block_rows):
            blocks_ref[index] = attention_ref[:, index * block_rows : (index + 1) * block_rows]

    for index, count in enumerate(piece_counts):
        parts = [refs.pop(0)[...] for _ in range(count)]
        piece = parts[0] if count == 1 else jnp.concatenate(parts, axis=0)
        part = jnp.dot(blocks_ref[order_ref[index]], piece, preferred_element_type=jnp.float32)
        acc = part if acc is None else acc + part
    if not final:
        out_ref[...] = acc
        return
    hidden_ref, control_ref, gate_ref = refs
    result = hidden_ref[...].astype(jnp.float32) + gate_ref[...].astype(jnp.float32) * acc
    out_ref[...] = (result + control_ref[...].astype(jnp.float32)).astype(jnp.bfloat16)


def project(attention, pieces, order, acc=None, residual=None):
    rows, channels = attention.shape
    block_rows = sum(p.shape[0] for p in pieces[0])
    model_width = pieces[0][0].shape[1]
    chunk = model_width // 4 if model_width % 512 == 0 else model_width
    col_block = lambda height: pl.BlockSpec((height, chunk), lambda n: (0, n))
    operands, specs = [], []
    if acc is not None:
        operands.append(acc)
        specs.append(col_block(rows))
    for parts in pieces:
        for part in parts:
            operands.append(part)
            specs.append(col_block(part.shape[0]))
    if residual is not None:
        hidden, control, gate = residual
        operands += [hidden, control, gate]
        specs += [col_block(rows), col_block(rows), col_block(1)]
    final = residual is not None
    return pl.pallas_call(
        lambda *refs: project_body(
            *refs,
            piece_counts=[len(parts) for parts in pieces],
            block_rows=block_rows,
            has_acc=acc is not None,
            final=final,
        ),
        grid=(model_width // chunk,),
        in_specs=[pl.BlockSpec(memory_space=pltpu.SMEM), pl.BlockSpec((rows, channels), lambda n: (0, 0))] + specs,
        out_specs=col_block(rows),
        out_shape=jax.ShapeDtypeStruct((rows, model_width), jnp.bfloat16 if final else jnp.float32),
        scratch_shapes=[pltpu.VMEM((channels // block_rows, rows, block_rows), jnp.bfloat16)],
        name="project_final" if final else "project_part",
    )(jnp.stack(order), attention, *operands)


def per_device(queries, keys, values, hidden, control, gate, out_weight):
    channels = queries.shape[-1]
    model_width = out_weight.shape[1]
    frames = lax.axis_size("frame")
    spaces = lax.axis_size("space")
    f = lax.axis_index("frame")
    s = lax.axis_index("space")
    tiles = window_tiles(keys.reshape(-1, channels), values.reshape(-1, channels))
    residual = (hidden.reshape(-1, model_width), control.reshape(-1, model_width), gate.reshape(1, -1))
    if frames == 4 and spaces == 2:
        core = lambda value: lax.ppermute(value, "frame", [(i, i ^ 1) for i in range(frames)])
        cross = lambda value: lax.ppermute(value, "frame", [(i, i ^ 2) for i in range(frames)])
        side = lambda value: lax.ppermute(value, "space", [(i, i ^ 1) for i in range(spaces)])
        half = out_weight.shape[0] // 2
        w_side = side(out_weight)
        w_cross = cross(out_weight)
        w_far = [cross(w_side[:half]), side(w_cross[half:])]
        near = [[out_weight], [core(out_weight)], [w_side], [core(w_side)], [w_cross], [core(w_cross)]]
        near_order = [
            f * 2 + s,
            (f ^ 1) * 2 + s,
            f * 2 + (s ^ 1),
            (f ^ 1) * 2 + (s ^ 1),
            (f ^ 2) * 2 + s,
            (f ^ 3) * 2 + s,
        ]
        far = [w_far, [core(w) for w in w_far]]
        far_order = [(f ^ 2) * 2 + (s ^ 1), (f ^ 3) * 2 + (s ^ 1)]
        attention = attend(queries.reshape(-1, channels), tiles)
        partial = project(attention, near, near_order)
        result = project(attention, far, far_order, acc=partial, residual=residual)
    else:
        whole = lax.all_gather(out_weight, ("frame", "space"), axis=0, tiled=True)
        attention = attend(queries.reshape(-1, channels), tiles)
        result = project(attention, [[whole]], [jnp.int32(0)], residual=residual)
    return result.reshape(hidden.shape)


def solution(mesh):
    tokens = P(("batch", "frame"), "space", None, None, None)
    return jax.shard_map(
        per_device,
        mesh=mesh,
        in_specs=(tokens, tokens, tokens, tokens, tokens, P(), P(("frame", "space"), None)),
        out_specs=tokens,
        check_vma=False,
    )
```
